8 devices in a mesh: rep: 1 (over z), fsdp: 8 (over y, x, core).
Axes of the slice: x: 2, y: 2, z: 1, core: 2. Of those that a mesh axis runs over, the one named last changes fastest.
Arguments:
- tokens: bfloat16 [16384, 4096], P(('rep', 'fsdp'))
- norm_w: float32 [2, 4096], replicated
- router_w: bfloat16 [2, 4096, 8], replicated
- w_gate: bfloat16 [2, 8, 4096, 1376], P(None, None, None, 'fsdp')
- w_up: bfloat16 [2, 8, 4096, 1376], P(None, None, None, 'fsdp')
- w_down: bfloat16 [2, 8, 1376, 4096], P(None, None, 'fsdp')
- route_ids: int32 [2, 16384, 2], P(None, ('rep', 'fsdp'))
Outputs:
- output: bfloat16 [16384, 4096], P(('rep', 'fsdp'))
All inputs are finite; a program needn't handle non-finite values.
Results may differ from the reference program's by a relative error of at most 0.0118026.
Values are sent between devices in bfloat16 or wider.
A program may use at most 1 GiB of HBM per device.

```python
import jax
import jax.numpy as jnp
from jax import lax

D = 4096
FF = 1376
EXPERTS = 8
TOP = 2
LAYERS = 2
TOKENS = 16384

NORM_EPS = 1e-5


def permute_one(one_key):
    return jax.random.permutation(one_key, EXPERTS)


def pick_rows(perm_row, rank_ids):
    return perm_row[rank_ids]


def draw_route(route_key):
    heavy_n = min(2, TOP - 1)
    light_n = EXPERTS - heavy_n
    window = TOP - heavy_n
    perm_key, rank_key = jax.random.split(route_key)
    perm_table = jax.vmap(permute_one)(jax.random.split(perm_key, LAYERS))
    rank_draws = jax.random.randint(rank_key, (3, LAYERS, TOKENS), 0, light_n)
    skewed = jnp.min(rank_draws, axis=0)
    tok_pos = jnp.arange(TOKENS)
    stride = max(TOKENS // light_n, 1)
    anchor = (tok_pos // stride) % light_n
    win_start = jnp.where((tok_pos % stride == 0)[None, :], anchor[None, :], skewed)
    light_ranks = heavy_n + (win_start[:, :, None] + jnp.arange(window)[None, None, :]) % light_n
    heavy_ranks = jnp.broadcast_to(jnp.arange(heavy_n), (LAYERS, TOKENS, heavy_n))
    rank_ids = jnp.concatenate([heavy_ranks, light_ranks], axis=2)
    return jax.vmap(pick_rows)(perm_table, rank_ids).astype(jnp.int32)


def setup_inputs(seed: int = 0, part: int = 0) -> dict:
    base_key, shared_key = jax.random.split(jax.random.key(seed))
    part_key = jax.random.fold_in(base_key, part)
    tok_key, route_key = jax.random.split(part_key)
    weight_keys = jax.random.split(shared_key, 5)
    tokens = jax.random.normal(tok_key, (TOKENS, D), jnp.float32).astype(jnp.bfloat16)
    norm_w = 1.0 + 0.25 * jax.random.normal(weight_keys[0], (LAYERS, D), jnp.float32)
    router_w = (1.5 * D ** -0.5 * jax.random.normal(weight_keys[1], (LAYERS, D, EXPERTS), jnp.float32)).astype(jnp.bfloat16)
    w_gate = (D ** -0.5 * jax.random.normal(weight_keys[2], (LAYERS, EXPERTS, D, FF), jnp.float32)).astype(jnp.bfloat16)
    w_up = (D ** -0.5 * jax.random.normal(weight_keys[3], (LAYERS, EXPERTS, D, FF), jnp.float32)).astype(jnp.bfloat16)
    w_down = (2.0 * FF ** -0.5 * jax.random.normal(weight_keys[4], (LAYERS, EXPERTS, FF, D), jnp.float32)).astype(jnp.bfloat16)
    route_ids = draw_route(route_key)
    return {"tokens": tokens, "norm_w": norm_w, "router_w": router_w, "w_gate": w_gate, "w_up": w_up, "w_down": w_down, "route_ids": route_ids}


def moe_layer(resid, norm_w, router_w, w_gate, w_up, w_down, route_ids):
    row_block = 128
    resid_f = resid.astype(jnp.float32)
    inv_rms = lax.rsqrt(jnp.mean(resid_f * resid_f, axis=-1, keepdims=True) + NORM_EPS)
    hidden = (resid_f * inv_rms * norm_w).astype(jnp.bfloat16)
    logits = jnp.dot(hidden, router_w, preferred_element_type=jnp.float32)
    gate_probs = jax.nn.softmax(jnp.take_along_axis(logits, route_ids, axis=1), axis=-1)
    flat_ids = route_ids.reshape(-1)
    n_rows = flat_ids.shape[0]
    sort_order = jnp.argsort(flat_ids, stable=True)
    counts = jnp.sum((flat_ids[:, None] == jnp.arange(EXPERTS, dtype=jnp.int32)[None, :]).astype(jnp.int32), axis=0)
    padded = (counts + row_block - 1) // row_block * row_block
    pad_end = jnp.cumsum(padded)
    pad_start = pad_end - padded
    grp_start = jnp.cumsum(counts) - counts
    n_blocks = (n_rows + EXPERTS * (row_block - 1)) // row_block + 1
    slot_pos = jnp.arange(n_blocks * row_block)
    slot_exp = jnp.minimum(jnp.searchsorted(pad_end, slot_pos, side="right"), EXPERTS - 1)
    within = slot_pos - pad_start[slot_exp]
    is_valid = within < counts[slot_exp]
    src_row = sort_order[jnp.clip(grp_start[slot_exp] + within, 0, n_rows - 1)]
    tok_idx = src_row // TOP
    weight = jnp.where(is_valid, gate_probs.reshape(-1)[src_row], 0.0)
    block_exp = slot_exp.reshape(n_blocks, row_block)[:, 0]

    def run_block(block_args):
        block_tok, expert = block_args
        gathered = hidden[block_tok]
        up_gate = jnp.dot(gathered, w_gate[expert], preferred_element_type=jnp.float32)
        up_lin = jnp.dot(gathered, w_up[expert], preferred_element_type=jnp.float32)
        act_bf16 = (jax.nn.silu(up_gate) * up_lin).astype(jnp.bfloat16)
        return jnp.dot(act_bf16, w_down[expert], preferred_element_type=jnp.float32)

    block_out = lax.map(run_block, (tok_idx.reshape(n_blocks, row_block), block_exp))
    contrib = block_out.reshape(-1, D) * weight[:, None]
    moe_sum = jnp.zeros((TOKENS, D), jnp.float32).at[tok_idx].add(contrib)
    return (resid_f + moe_sum).astype(jnp.bfloat16)


def reference(tokens, norm_w, router_w, w_gate, w_up, w_down, route_ids):
    def layer_step(resid, layer_args):
        norm_l, router_l, gate_l, up_l, down_l, route_l = layer_args
        return moe_layer(resid, norm_l, router_l, gate_l, up_l, down_l, route_l), None

    final_x, _ = lax.scan(layer_step, tokens, (norm_w, router_w, w_gate, w_up, w_down, route_ids))
    return final_x
```

```python
import functools

import jax
import jax.numpy as jnp
from jax import lax
from jax.experimental import pallas as pl
from jax.experimental.pallas import tpu as pltpu
from jax.sharding import PartitionSpec as P


EPS = 1e-5
TM = 256
DC = 256
NG = 4
CAP = 256
SIDE_RANKS = {4: ((4, 7), (5, 6)), 2: ((2, 5, 7), (3, 4, 6))}
VMEM = 66 * 1000 * 1000


def pad16(n):
    return (n + 15) // 16 * 16


def prep_body(groups, n_exp, s_ref, *refs):
    srcs, outs, sel = refs[:3], refs[3:-1], refs[-1]
    n = sum(groups)
    wide = sel.shape[0] // n

    @pl.when(pl.program_id(0) == 0)
    def _():
        col = lax.broadcasted_iota(jnp.int32, (wide, sel.shape[1]), 1)
        line = lax.broadcasted_iota(jnp.int32, (wide, sel.shape[1]), 0)
        for k in range(n):
            sel[k * wide:(k + 1) * wide, :] = (col == line * n_exp + s_ref[k]).astype(jnp.bfloat16)

    for m in range(3):
        k = 0
        for out, size in zip(outs, groups):
            for j in range(size):
                out[j, m] = jnp.dot(sel[k * wide:(k + 1) * wide, :], srcs[m][0], preferred_element_type=jnp.float32).astype(jnp.bfloat16)
                k += 1


def prep(layer, experts, groups, w_gate, w_up, w_down):
    n_exp, width, inner = w_gate.shape[1:]
    wide = pad16(inner)
    lines = [jnp.transpose(w, order).reshape(w.shape[0], inner * n_exp, width) for w, order in ((w_gate, (0, 3, 1, 2)), (w_up, (0, 3, 1, 2)), (w_down, (0, 2, 1, 3)))]
    n = sum(groups)
    return pl.pallas_call(
        functools.partial(prep_body, groups, n_exp),
        out_shape=[jax.ShapeDtypeStruct((g, 3, wide, width), jnp.bfloat16) for g in groups],
        grid_spec=pltpu.PrefetchScalarGridSpec(
            num_scalar_prefetch=1,
            grid=(width // DC,),
            in_specs=[pl.BlockSpec((1, inner * n_exp, DC), lambda c, s: (layer, 0, c))] * 3,
            out_specs=[pl.BlockSpec((g, 3, wide, DC), lambda c, s: (0, 0, 0, c)) for g in groups],
            scratch_shapes=[pltpu.VMEM((n * wide, inner * n_exp), jnp.bfloat16)],
        ),
        compiler_params=pltpu.CompilerParams(vmem_limit_bytes=VMEM),
        cost_estimate=pl.CostEstimate(flops=n * 600_000_000, bytes_accessed=70_000_000 + n * 4_300_000, transcendentals=0),
        name="prep",
    )(experts, *lines)


def expert_body(pieces, n_w, aliased, s_ref, h_ref, *refs):
    w_refs = refs[:n_w]
    o_ref = refs[n_w + (1 if aliased else 0)]
    w1, w3, w2, act, sems = refs[n_w + (2 if aliased else 1):]
    wide = w1.shape[0] // len(pieces)
    i = pl.program_id(0)

    def copies(m, dst):
        out = []
        for p, (r, lead) in enumerate(pieces):
            src = w_refs[r].at[lead + (m,)] if isinstance(lead, tuple) else w_refs[r].at[lead, m]
            out.append(pltpu.make_async_copy(src, dst.at[pl.ds(p * wide, wide)], sems.at[m, p]))
        return out

    @pl.when(i == 0)
    def _():
        for m, dst in enumerate((w1, w3, w2)):
            for c in copies(m, dst):
                c.start()
        for m, dst in enumerate((w1, w3)):
            for c in copies(m, dst):
                c.wait()

    nt = (((1,), (1,)), ((), ()))

    @pl.when(i < s_ref[1])
    def _():
        cols = w1.shape[0]
        steps = (cols + 255) // 256

        def up(c, carry):
            at = pl.multiple_of(jnp.minimum(c * 256, cols - 256), 128)
            h = h_ref[...]
            u = lax.dot_general(h, w1[pl.ds(at, 256), :], nt, preferred_element_type=jnp.float32)
            v = lax.dot_general(h, w3[pl.ds(at, 256), :], nt, preferred_element_type=jnp.float32)
            act[:, pl.ds(at, 256)] = (jax.nn.silu(u) * v).astype(jnp.bfloat16)
            return carry

        lax.fori_loop(0, steps, up, 0)

    @pl.when(i == 0)
    def _():
        for c in copies(2, w2):
            c.wait()

    @pl.when(i < s_ref[1])
    def _():
        def down(c, carry):
            at = pl.multiple_of(c * 512, 512)
            o_ref[:, pl.ds(at, 512)] = jnp.dot(act[...], w2[:, pl.ds(at, 512)], preferred_element_type=jnp.float32)
            return carry

        lax.fori_loop(0, o_ref.shape[1] // 512, down, 0)


def expert(scalars, rows, weights, pieces, out, max_tiles, out_rows):
    width = rows.shape[1]
    wide = weights[0].shape[-2]
    cols = wide * len(pieces)
    aliased = out is not None
    at = lambda i, s: (s[0] + jnp.minimum(i, s[1] - 1), 0)
    to = lambda i, s: (s[2] + jnp.minimum(i, s[1] - 1), 0)
    anywhere = pl.BlockSpec(memory_space=pl.ANY)
    return pl.pallas_call(
        functools.partial(expert_body, pieces, len(weights), aliased),
        out_shape=jax.ShapeDtypeStruct((out_rows, width), jnp.float32),
        grid_spec=pltpu.PrefetchScalarGridSpec(
            num_scalar_prefetch=1,
            grid=(max_tiles,),
            in_specs=[pl.BlockSpec((TM, width), at)] + [anywhere] * (len(weights) + aliased),
            out_specs=pl.BlockSpec((TM, width), to),
            scratch_shapes=[pltpu.VMEM((cols, width), jnp.bfloat16)] * 3
            + [pltpu.VMEM((TM, cols), jnp.bfloat16), pltpu.SemaphoreType.DMA((3, len(pieces)))],
        ),
        input_output_aliases={2 + len(weights): 0} if aliased else {},
        compiler_params=pltpu.CompilerParams(vmem_limit_bytes=VMEM),
        cost_estimate=pl.CostEstimate(flops=3_000_000_000, bytes_accessed=60_000_000, transcendentals=0),
        name="expert",
    )(scalars, rows, *weights, *((out,) if aliased else ()))


def prefix(onehot):
    n, k = onehot.shape
    blocks = onehot.astype(jnp.float32).reshape(n // 128, 128, k)
    lower = (jnp.arange(128)[:, None] > jnp.arange(128)[None, :]).astype(jnp.float32)
    inside = jnp.einsum("ij,bjk->bik", lower, blocks)
    sums = blocks.sum(axis=1)
    nb = n // 128
    before = jnp.einsum("ij,jk->ik", (jnp.arange(nb)[:, None] > jnp.arange(nb)[None, :]).astype(jnp.float32), sums)
    return (inside + before[:, None, :]).reshape(n, k).astype(jnp.int32), sums.sum(axis=0).astype(jnp.int32)


def row_plan(slot0, slot1, n_local):
    n_tok = slot0.shape[0]
    flat = jnp.concatenate([slot0, slot1])
    onehot = flat[:, None] == jnp.arange(n_local)[None, :]
    within, counts = prefix(onehot)
    tiles = jnp.maximum((counts + TM - 1) // TM, 1)
    lower = jnp.arange(n_local)[:, None] > jnp.arange(n_local)[None, :]
    first = jnp.sum(jnp.where(lower, tiles[None, :], 0), axis=1)
    pos = jnp.sum(jnp.where(onehot, within + first[None, :] * TM, 0), axis=1)
    n = 2 * n_tok
    spare = jnp.where(jnp.arange(TM)[None, :] < (tiles * TM - counts)[:, None], jnp.arange(n_local)[:, None], n_local)
    keys = jnp.concatenate([flat, spare.reshape(-1)])
    order = lax.sort(keys * 8192 + jnp.arange(keys.shape[0], dtype=jnp.int32)) & 8191
    token = jnp.where(order < n, order % n_tok, 0)
    scalars = jnp.stack([first, tiles, first], axis=1).astype(jnp.int32)
    return token, pos[:n_tok], pos[n_tok:], scalars


def pick(table, index, size):
    return jnp.sum(jnp.where(index[..., None] == jnp.arange(size), table, 0), axis=-1)


def norm_gates(x, norm_w, router_w, ids0, ids1):
    xf = x.astype(jnp.float32)
    inv = lax.rsqrt(jnp.mean(xf * xf, axis=-1, keepdims=True) + EPS)
    h = (xf * inv * norm_w).astype(jnp.bfloat16)
    r = jnp.dot(h, router_w, preferred_element_type=jnp.float32)
    n_exp = router_w.shape[1]
    r0 = jnp.sum(jnp.where(ids0[:, None] == jnp.arange(n_exp), r, 0.0), axis=-1)
    r1 = jnp.sum(jnp.where(ids1[:, None] == jnp.arange(n_exp), r, 0.0), axis=-1)
    g = jax.nn.softmax(jnp.stack([r0, r1], axis=-1), axis=-1)
    return h, g[:, :1], g[:, 1:]


def take(table, index):
    return table.at[index].get(mode="promise_in_bounds")


def weighed(out, pos, gate, here):
    return jnp.where(here[:, None], gate * take(out, jnp.where(here, pos, 0)), 0.0)


def solution(mesh):
    n_dev = mesh.shape["fsdp"]

    def hop(a, bit):
        return lax.ppermute(a, "fsdp", [(i, i ^ bit) for i in range(n_dev)])

    def general(x, norm_w, router_w, w_gate, w_up, w_down, ids):
        n_layers, n_exp = w_gate.shape[:2]
        n_tok = x.shape[0]
        for l in range(n_layers):
            token, pos0, pos1, scalars = row_plan(ids[l, 0], ids[l, 1], n_exp)
            h, g0, g1 = norm_gates(x, norm_w[l], router_w[l], ids[l, 0], ids[l, 1])
            rows = take(h, token)

            def step(e, out, l=l, rows=rows, scalars=scalars):
                w = prep(l, e[None].astype(jnp.int32), (1,), w_gate, w_up, w_down)[0][0]
                full = lax.all_gather(w, "fsdp")
                s = lax.dynamic_index_in_dim(scalars, e, 0, keepdims=False)
                return expert(s, rows, [full], [(0, p) for p in range(n_dev)], out, n_tok // TM, rows.shape[0])

            out = lax.fori_loop(0, n_exp, step, jnp.zeros(rows.shape, jnp.float32))
            x = (x.astype(jnp.float32) + (g0 * take(out, pos0) + g1 * take(out, pos1))).astype(jnp.bfloat16)
        return x

    def local_fn(tokens, norm_w, router_w, w_gate, w_up, w_down, route_ids):
        n_layers, n_exp = w_gate.shape[:2]
        n_tok = tokens.shape[0]
        n_light = (n_exp - NG) // 2
        n_local = NG + n_light
        me = lax.axis_index("fsdp")
        ids = jnp.swapaxes(route_ids, 1, 2)
        every = lax.all_gather(ids, "fsdp")
        hits = every[..., None] == jnp.arange(n_exp)
        load = jnp.sum(hits.astype(jnp.int32), axis=(0, 2, 3))
        earlier = jnp.arange(n_exp)[None, :] < jnp.arange(n_exp)[:, None]
        ahead = (load[:, None, :] > load[:, :, None]) | ((load[:, None, :] == load[:, :, None]) & earlier[None])
        rank = jnp.sum(ahead.astype(jnp.int32), axis=2)
        by_rank = jnp.sum(jnp.where(rank[:, None, :] == jnp.arange(n_exp)[None, :, None], jnp.arange(n_exp), 0), axis=2).astype(jnp.int32)
        home_of = [-1] * (NG - 1) + [-2] + [0] * (n_exp - NG)
        local_of = list(range(n_exp))
        for side, ranks in enumerate(SIDE_RANKS[NG]):
            for j, k in enumerate(ranks):
                home_of[k], local_of[k] = side, NG + j
        home = pick(jnp.array(home_of), rank, n_exp)
        local = pick(jnp.array(local_of), rank, n_exp)
        at_home = jnp.sum(jnp.where(hits, home[None, :, None, None, :], 0), axis=-1)
        lend = [n_dev // 2 if l % 2 == 0 else n_dev // 4 for l in range(n_layers)]
        share = [n_dev // 4 if l % 2 == 0 else n_dev // 2 for l in range(n_layers)]
        side_of = jnp.stack([(jnp.arange(n_dev) // bit) % 2 for bit in lend], axis=1)
        mine_side = jnp.stack([(me // bit) % 2 for bit in lend])
        needs = [jnp.any(at_home == v, axis=2) for v in (0, 1)]
        late = jnp.any(at_home == -2, axis=2)
        lent = jnp.where(side_of[:, :, None] == 0, needs[1], needs[0])
        n_lent = jnp.sum(lent.astype(jnp.int32), axis=2)
        ok = jnp.all(n_lent <= CAP) & ~jnp.any(needs[0] & needs[1]) & ~jnp.any(lent & late)

        def adaptive(x, norm_w, router_w, w_gate, w_up, w_down, ids):
            mine = lax.dynamic_index_in_dim(every, me, 0, keepdims=False)
            my_local = jnp.sum(jnp.where(mine[..., None] == jnp.arange(n_exp), local[:, None, None, :], 0), axis=-1)
            my_lent = lax.dynamic_index_in_dim(lent, me, 0, keepdims=False)
            sides = [jnp.array(r) for r in SIDE_RANKS[NG]]
            ones = (1,) * (NG - 1)
            chosen = [[jnp.where(mine_side[l] == v, by_rank[l][sides[0]], by_rank[l][sides[1]]) for v in (0, 1)] for l in range(n_layers)]

            def gathers(l, heavy, light):
                first = prep(l, heavy[:1], (1,), w_gate, w_up, w_down)
                rest = prep(l, jnp.concatenate([heavy[1:NG], light]), ones + (n_light, n_light), w_gate, w_up, w_down)
                return [lax.all_gather(w[0], "fsdp") for w in first + rest[:NG - 1]], *rest[NG - 1:]

            full, own, other = gathers(0, by_rank[0], jnp.concatenate(chosen[0]))
            own_x, sent = hop(own, share[0]), hop(other, lend[0])
            for l in range(n_layers):
                key = jnp.where(my_lent[l], 0, 8192) + jnp.arange(n_tok, dtype=jnp.int32)
                code = (my_local[l, 0] * 16 + my_local[l, 1]) * 64 + mine[l, 0] * 8 + mine[l, 1]
                code = jnp.where(my_lent[l], code, (n_local * 16 + n_local) * 64)
                key, code = lax.sort((key, code), num_keys=1)
                place = jnp.minimum(prefix(my_lent[l][:, None])[0][:, 0], CAP - 1)
                code = hop(code[:CAP], lend[l])
                ids0 = jnp.concatenate([mine[l, 0], code // 8 % 8])
                ids1 = jnp.concatenate([mine[l, 1], code % 8])
                slot0 = jnp.concatenate([jnp.where(my_lent[l], n_local, my_local[l, 0]), code // 1024])
                slot1 = jnp.concatenate([jnp.where(my_lent[l], n_local, my_local[l, 1]), code // 64 % 16])
                token, pos0, pos1, scalars = row_plan(slot0, slot1, n_local)
                guest = hop(take(x, (key & 8191)[:CAP]), lend[l])
                both = jnp.concatenate([x, guest])
                h, g0, g1 = norm_gates(both, norm_w[l], router_w[l], ids0, ids1)
                rows = take(h, token)
                max_tiles = (n_tok + CAP) // TM
                whole = [(0, p) for p in range(n_dev)]
                gathered = lambda k, out: expert(scalars[k], rows, [full[k]], whole, out, max_tiles, rows.shape[0])
                if l:
                    far = hop(sent, share[l])
                    beside = [hop(w, 1) for w in (own, own_x, sent)]
                    out = gathered(0, None)
                else:
                    out = gathered(0, None)
                    own_x, sent, out = lax.optimization_barrier((own_x, sent, out))
                    far = hop(sent, share[l])
                    beside = [hop(w, 1) for w in (own, own_x, sent)]
                if l + 1 < n_layers:
                    heavy, light, out = lax.optimization_barrier((by_rank[l + 1], jnp.concatenate(chosen[l + 1]), out))
                    coming, own2, other2 = gathers(l + 1, heavy, light)
                for k in range(1, NG - 1):
                    out = gathered(k, out)
                far, out = lax.optimization_barrier((far, out))
                eight = [own, own_x, sent, far] + beside + [hop(far, 1)]
                if l + 1 < n_layers:
                    own2, other2, _ = lax.optimization_barrier((own2, other2, far))
                    own_x2, sent2 = hop(own2, share[l + 1]), hop(other2, lend[l + 1])
                for j in range(n_light):
                    out = expert(scalars[NG + j], rows, eight, [(p, j) for p in range(n_dev)], out, max_tiles, rows.shape[0])
                last = NG - 1
                here0, here1 = slot0 != last, slot1 != last
                part = both.astype(jnp.float32) + (weighed(out, pos0, g0, here0) + weighed(out, pos1, g1, here1))
                back = hop(part[n_tok:].astype(jnp.bfloat16), lend[l])
                part = jnp.where(my_lent[l][:, None], take(back, place).astype(jnp.float32), part[:n_tok])
                part, late_full = lax.optimization_barrier((part, full[last]))
                at_last = scalars[last] * jnp.array([1, 1, 0])
                final = expert(at_last, rows, [late_full], whole, None, max_tiles, n_tok)
                use0, use1 = ~here0[:n_tok], ~here1[:n_tok]
                pos = jnp.where(use0, pos0[:n_tok], pos1[:n_tok]) - scalars[last, 0] * TM
                gate = jnp.where(use0[:, None], g0[:n_tok], g1[:n_tok])
                x = (part + weighed(final, pos, gate, use0 | use1)).astype(jnp.bfloat16)
                if l + 1 < n_layers:
                    x, own_x2, sent2 = lax.optimization_barrier((x, own_x2, sent2))
                    full, own, own_x, sent = coming, own2, own_x2, sent2
            return x

        return lax.cond(ok, adaptive, general, tokens, norm_w, router_w, w_gate, w_up, w_down, ids)

    row_spec = P(("rep", "fsdp"), None)
    col_spec = P(None, None, None, "fsdp")
    return jax.shard_map(
        local_fn,
        mesh=mesh,
        in_specs=(row_spec, P(), P(), col_spec, col_spec, P(None, None, "fsdp", None), P(None, ("rep", "fsdp"), None)),
        out_specs=row_spec,
        check_vma=False,
    )
```

```python
import functools

import jax
import jax.numpy as jnp
from jax import lax
from jax.experimental import pallas as pl
from jax.experimental.pallas import tpu as pltpu
from jax.sharding import PartitionSpec as P


EPS = 1e-5
TM = 256
DC = 256
NG = 4
CAP = 256
SIDE_RANKS = {4: ((4, 7), (5, 6)), 2: ((2, 5, 7), (3, 4, 6))}
VMEM = 66 * 1000 * 1000


def pad16(n):
    return (n + 15) // 16 * 16


def prep_body(groups, n_exp, s_ref, *refs):
    srcs, outs, sel = refs[:3], refs[3:-1], refs[-1]
    n = sum(groups)
    wide = sel.shape[0] // n

    @pl.when(pl.program_id(0) == 0)
    def _():
        col = lax.broadcasted_iota(jnp.int32, (wide, sel.shape[1]), 1)
        line = lax.broadcasted_iota(jnp.int32, (wide, sel.shape[1]), 0)
        for k in range(n):
            sel[k * wide:(k + 1) * wide, :] = (col == line * n_exp + s_ref[k]).astype(jnp.bfloat16)

    for m in range(3):
        k = 0
        for out, size in zip(outs, groups):
            for j in range(size):
                out[j, m] = jnp.dot(sel[k * wide:(k + 1) * wide, :], srcs[m][0], preferred_element_type=jnp.float32).astype(jnp.bfloat16)
                k += 1


def prep(layer, experts, groups, w_gate, w_up, w_down):
    n_exp, width, inner = w_gate.shape[1:]
    wide = pad16(inner)
    lines = [jnp.transpose(w, order).reshape(w.shape[0], inner * n_exp, width) for w, order in ((w_gate, (0, 3, 1, 2)), (w_up, (0, 3, 1, 2)), (w_down, (0, 2, 1, 3)))]
    n = sum(groups)
    return pl.pallas_call(
        functools.partial(prep_body, groups, n_exp),
        out_shape=[jax.ShapeDtypeStruct((g, 3, wide, width), jnp.bfloat16) for g in groups],
        grid_spec=pltpu.PrefetchScalarGridSpec(
            num_scalar_prefetch=1,
            grid=(width // DC,),
            in_specs=[pl.BlockSpec((1, inner * n_exp, DC), lambda c, s: (layer, 0, c))] * 3,
            out_specs=[pl.BlockSpec((g, 3, wide, DC), lambda c, s: (0, 0, 0, c)) for g in groups],
            scratch_shapes=[pltpu.VMEM((n * wide, inner * n_exp), jnp.bfloat16)],
        ),
        compiler_params=pltpu.CompilerParams(vmem_limit_bytes=VMEM),
        cost_estimate=pl.CostEstimate(flops=n * 600_000_000, bytes_accessed=70_000_000 + n * 4_300_000, transcendentals=0),
        name="prep",
    )(experts, *lines)


def expert_body(pieces, n_w, aliased, added, s_ref, h_ref, *refs):
    w_refs = refs[:n_w]
    more = n_w + aliased + 2 * added
    o_ref = refs[more]
    w1, w3, w2, act, sems = refs[more + 1:]
    wide = w1.shape[0] // len(pieces)
    i = pl.program_id(0)

    def copies(m, dst):
        out = []
        for p, (r, lead) in enumerate(pieces):
            src = w_refs[r].at[lead + (m,)] if isinstance(lead, tuple) else w_refs[r].at[lead, m]
            out.append(pltpu.make_async_copy(src, dst.at[pl.ds(p * wide, wide)], sems.at[m, p]))
        return out

    @pl.when(i == 0)
    def _():
        for m, dst in enumerate((w1, w3, w2)):
            for c in copies(m, dst):
                c.start()
        for m, dst in enumerate((w1, w3)):
            for c in copies(m, dst):
                c.wait()

    nt = (((1,), (1,)), ((), ()))

    @pl.when(i < s_ref[1])
    def _():
        cols = w1.shape[0]
        steps = (cols + 255) // 256

        def up(c, carry):
            at = pl.multiple_of(jnp.minimum(c * 256, cols - 256), 128)
            h = h_ref[...]
            u = lax.dot_general(h, w1[pl.ds(at, 256), :], nt, preferred_element_type=jnp.float32)
            v = lax.dot_general(h, w3[pl.ds(at, 256), :], nt, preferred_element_type=jnp.float32)
            act[:, pl.ds(at, 256)] = (jax.nn.silu(u) * v).astype(jnp.bfloat16)
            return carry

        lax.fori_loop(0, steps, up, 0)

    @pl.when(i == 0)
    def _():
        for c in copies(2, w2):
            c.wait()

    @pl.when(i < s_ref[1])
    def _():
        def down(c, carry):
            at = pl.multiple_of(c * 512, 512)
            o = jnp.dot(act[...], w2[:, pl.ds(at, 512)], preferred_element_type=jnp.float32)
            if added:
                x_ref, gate_ref = refs[more - 2:more]
                o = x_ref[:, pl.ds(at, 512)].astype(jnp.float32) + gate_ref[...] * o
            o_ref[:, pl.ds(at, 512)] = o
            return carry

        lax.fori_loop(0, o_ref.shape[1] // 512, down, 0)


def expert(scalars, rows, weights, pieces, out, max_tiles, add=None):
    width = rows.shape[1]
    wide = weights[0].shape[-2]
    cols = wide * len(pieces)
    aliased = out is not None
    at = lambda i, s: (s[0] + jnp.minimum(i, s[1] - 1), 0)
    anywhere = pl.BlockSpec(memory_space=pl.ANY)
    return pl.pallas_call(
        functools.partial(expert_body, pieces, len(weights), aliased, add is not None),
        out_shape=jax.ShapeDtypeStruct(rows.shape, jnp.float32),
        grid_spec=pltpu.PrefetchScalarGridSpec(
            num_scalar_prefetch=1,
            grid=(max_tiles,),
            in_specs=[pl.BlockSpec((TM, width), at)] + [anywhere] * (len(weights) + aliased)
            + ([pl.BlockSpec((TM, width), at), pl.BlockSpec((TM, 1), at)] if add else []),
            out_specs=pl.BlockSpec((TM, width), at),
            scratch_shapes=[pltpu.VMEM((cols, width), jnp.bfloat16)] * 3
            + [pltpu.VMEM((TM, cols), jnp.bfloat16), pltpu.SemaphoreType.DMA((3, len(pieces)))],
        ),
        input_output_aliases={2 + len(weights): 0} if aliased else {},
        compiler_params=pltpu.CompilerParams(vmem_limit_bytes=VMEM),
        cost_estimate=pl.CostEstimate(flops=3_000_000_000, bytes_accessed=60_000_000, transcendentals=0),
        name="expert",
    )(scalars, rows, *weights, *((out,) if aliased else ()), *(add or ()))


def prefix(onehot):
    n, k = onehot.shape
    blocks = onehot.astype(jnp.float32).reshape(n // 128, 128, k)
    lower = (jnp.arange(128)[:, None] > jnp.arange(128)[None, :]).astype(jnp.float32)
    inside = jnp.einsum("ij,bjk->bik", lower, blocks)
    sums = blocks.sum(axis=1)
    nb = n // 128
    before = jnp.einsum("ij,jk->ik", (jnp.arange(nb)[:, None] > jnp.arange(nb)[None, :]).astype(jnp.float32), sums)
    return (inside + before[:, None, :]).reshape(n, k).astype(jnp.int32), sums.sum(axis=0).astype(jnp.int32)


def row_plan(slots, n_local):
    n = slots.shape[0]
    onehot = slots[:, None] == jnp.arange(n_local)[None, :]
    within, counts = prefix(onehot)
    tiles = jnp.maximum((counts + TM - 1) // TM, 1)
    lower = jnp.arange(n_local)[:, None] > jnp.arange(n_local)[None, :]
    first = jnp.sum(jnp.where(lower, tiles[None, :], 0), axis=1)
    pos = jnp.sum(jnp.where(onehot, within + first[None, :] * TM, 0), axis=1)
    spare = jnp.where(jnp.arange(TM)[None, :] < (tiles * TM - counts)[:, None], jnp.arange(n_local)[:, None], n_local)
    keys = jnp.concatenate([slots, spare.reshape(-1)])
    order = lax.sort(keys * 8192 + jnp.arange(keys.shape[0], dtype=jnp.int32)) & 8191
    scalars = jnp.stack([first, tiles], axis=1).astype(jnp.int32)
    return jnp.where(order < n, order, 0), pos, scalars


def pick(table, index, size):
    return jnp.sum(jnp.where(index[..., None] == jnp.arange(size), table, 0), axis=-1)


def norm_gates(x, norm_w, router_w, ids0, ids1):
    xf = x.astype(jnp.float32)
    inv = lax.rsqrt(jnp.mean(xf * xf, axis=-1, keepdims=True) + EPS)
    h = (xf * inv * norm_w).astype(jnp.bfloat16)
    r = jnp.dot(h, router_w, preferred_element_type=jnp.float32)
    n_exp = router_w.shape[1]
    r0 = jnp.sum(jnp.where(ids0[:, None] == jnp.arange(n_exp), r, 0.0), axis=-1)
    r1 = jnp.sum(jnp.where(ids1[:, None] == jnp.arange(n_exp), r, 0.0), axis=-1)
    g = jax.nn.softmax(jnp.stack([r0, r1], axis=-1), axis=-1)
    return h, g[:, :1], g[:, 1:]


def take(table, index):
    return table.at[index].get(mode="promise_in_bounds")


def solution(mesh):
    n_dev = mesh.shape["fsdp"]

    def hop(a, bit):
        return lax.ppermute(a, "fsdp", [(i, i ^ bit) for i in range(n_dev)])

    def general(x, norm_w, router_w, w_gate, w_up, w_down, ids):
        n_layers, n_exp = w_gate.shape[:2]
        n_tok = x.shape[0]
        for l in range(n_layers):
            slot, pos, scalars = row_plan(jnp.concatenate([ids[l, 0], ids[l, 1]]), n_exp)
            h, g0, g1 = norm_gates(x, norm_w[l], router_w[l], ids[l, 0], ids[l, 1])
            rows = take(h, slot % n_tok)

            def step(e, out, l=l, rows=rows, scalars=scalars):
                w = prep(l, e[None].astype(jnp.int32), (1,), w_gate, w_up, w_down)[0][0]
                full = lax.all_gather(w, "fsdp")
                s = lax.dynamic_index_in_dim(scalars, e, 0, keepdims=False)
                return expert(s, rows, [full], [(0, p) for p in range(n_dev)], out, n_tok // TM)

            out = lax.fori_loop(0, n_exp, step, jnp.zeros(rows.shape, jnp.float32))
            x = (x.astype(jnp.float32) + (g0 * take(out, pos[:n_tok]) + g1 * take(out, pos[n_tok:]))).astype(jnp.bfloat16)
        return x

    def local_fn(tokens, norm_w, router_w, w_gate, w_up, w_down, route_ids):
        n_layers, n_exp = w_gate.shape[:2]
        n_tok = tokens.shape[0]
        n_light = (n_exp - NG) // 2
        n_local = NG + n_light
        me = lax.axis_index("fsdp")
        ids = jnp.swapaxes(route_ids, 1, 2)
        every = lax.all_gather(ids, "fsdp")
        hits = every[..., None] == jnp.arange(n_exp)
        load = jnp.sum(hits.astype(jnp.int32), axis=(0, 2, 3))
        earlier = jnp.arange(n_exp)[None, :] < jnp.arange(n_exp)[:, None]
        ahead = (load[:, None, :] > load[:, :, None]) | ((load[:, None, :] == load[:, :, None]) & earlier[None])
        rank = jnp.sum(ahead.astype(jnp.int32), axis=2)
        by_rank = jnp.sum(jnp.where(rank[:, None, :] == jnp.arange(n_exp)[None, :, None], jnp.arange(n_exp), 0), axis=2).astype(jnp.int32)
        home_of = [-1] * NG + [0] * (n_exp - NG)
        local_of = list(range(n_exp))
        for side, ranks in enumerate(SIDE_RANKS[NG]):
            for j, k in enumerate(ranks):
                home_of[k], local_of[k] = side, NG + j
        home = pick(jnp.array(home_of), rank, n_exp)
        local = pick(jnp.array(local_of), rank, n_exp)
        at_home = jnp.sum(jnp.where(hits, home[None, :, None, None, :], 0), axis=-1)
        lend = [n_dev // 2 if l % 2 == 0 else n_dev // 4 for l in range(n_layers)]
        share = [n_dev // 4 if l % 2 == 0 else n_dev // 2 for l in range(n_layers)]
        side_of = jnp.stack([(jnp.arange(n_dev) // bit) % 2 for bit in lend], axis=1)
        mine_side = jnp.stack([(me // bit) % 2 for bit in lend])
        needs = [jnp.any(at_home == v, axis=2) for v in (0, 1)]
        top = jnp.sum(jnp.where(rank == 0, jnp.arange(n_exp), 0), axis=1)[None, :, None, None]
        shared = jnp.all(jnp.any(every == top, axis=2))
        lent = jnp.where(side_of[:, :, None] == 0, needs[1], needs[0])
        n_lent = jnp.sum(lent.astype(jnp.int32), axis=2)
        ok = jnp.all(n_lent <= CAP) & shared

        def adaptive(x, norm_w, router_w, w_gate, w_up, w_down, ids):
            mine = lax.dynamic_index_in_dim(every, me, 0, keepdims=False)
            my_lent = lax.dynamic_index_in_dim(lent, me, 0, keepdims=False)
            my_top = jnp.sum(jnp.where(rank == 0, jnp.arange(n_exp), 0), axis=1)
            mine = jnp.where(mine[:, 0] == my_top[:, None], mine[:, 1], mine[:, 0])
            my_local = pick(local[:, None, :], mine, n_exp)
            sides = [jnp.array(r) for r in SIDE_RANKS[NG]]
            chosen = [[jnp.where(mine_side[l] == v, by_rank[l][sides[0]], by_rank[l][sides[1]]) for v in (0, 1)] for l in range(n_layers)]

            picks = [(by_rank[l, :1], jnp.concatenate([by_rank[l, 1:NG], *chosen[l]])) for l in range(n_layers)]
            picks = lax.optimization_barrier(picks)

            def shards(l, top, others):
                first = prep(l, top, (1,), w_gate, w_up, w_down)
                rest = prep(l, others, (1,) * (NG - 1 + 2 * n_light), w_gate, w_up, w_down)
                rest = [w[0] for w in rest]
                return first[0][0], rest[:NG - 1], rest[NG - 1:NG - 1 + n_light], rest[NG - 1 + n_light:]

            def all_of(w):
                return lax.all_gather(w, "fsdp")

            def after(values, *waited):
                return lax.optimization_barrier((values, *waited))[0]

            top_w, heavy_w, own, other = shards(0, *picks[0])
            full = [all_of(top_w)] + [all_of(w) for w in heavy_w]
            lists = []
            for l in range(n_layers):
                key = jnp.where(my_lent[l], 0, 8192) + jnp.arange(n_tok, dtype=jnp.int32)
                key, code = lax.sort((key, jnp.where(my_lent[l], my_local[l] * 8 + mine[l], n_local * 8)), num_keys=1)
                place = jnp.minimum(prefix(my_lent[l][:, None])[0][:, 0], CAP - 1)
                code = hop(code[:CAP], lend[l])
                lists.append(((key & 8191)[:CAP], place, code))
            for l in range(n_layers):
                key, place, code = lists[l]
                guest = hop(take(x, key), lend[l])
                if l == 0:
                    own_x, sent = [hop(w, share[0]) for w in own], [hop(w, lend[0]) for w in other]
                both = jnp.concatenate([x, guest])
                ids1 = jnp.concatenate([mine[l], code % 8])
                slots = jnp.concatenate([jnp.where(my_lent[l], n_local, my_local[l]), code // 8]) - 1
                slots = jnp.where(slots < 0, n_local - 1, slots)
                token, pos, scalars = row_plan(slots, n_local - 1)
                h, g0, g1 = norm_gates(both, norm_w[l], router_w[l], jnp.broadcast_to(my_top[l], ids1.shape), ids1)
                rows = take(h, token)
                max_tiles = (n_tok + CAP) // TM
                whole = [(0, p) for p in range(n_dev)]
                gathered = lambda k, out, w: expert(scalars[k - 1], rows, [w], whole, out, max_tiles)
                if l:
                    far = [hop(w, share[l]) for w in sent]
                    beside = [[hop(w, 1) for w in ws] for ws in zip(own, own_x, sent)]
                acc = expert(jnp.array([0, max_tiles], jnp.int32), h, [full[0]], whole, None, max_tiles, add=(both, g0))
                rows = after(rows, acc)
                if l == 0:
                    own_x, sent = after((own_x, sent), acc)
                    far = [hop(w, share[l]) for w in sent]
                    beside = [[hop(w, 1) for w in ws] for ws in zip(own, own_x, sent)]
                if l + 1 < n_layers:
                    top_w, heavy_w, own2, other2 = shards(l + 1, *after(picks[l + 1], acc))
                    coming = [all_of(top_w)] + [all_of(w) for w in heavy_w]
                    own_x2, sent2 = [hop(w, share[l + 1]) for w in own2], [hop(w, lend[l + 1]) for w in other2]
                out = None
                for k in range(1, NG - 1):
                    out = gathered(k, out, full[k])
                far = after(far, acc if out is None else out)
                for j in range(n_light):
                    w8 = [own[j], own_x[j], sent[j], far[j]] + beside[j] + [hop(far[j], 1)]
                    out = expert(scalars[NG - 1 + j], rows, w8, [(p, ()) for p in range(n_dev)], out, max_tiles)
                seen = acc[n_tok:] + g1[n_tok:] * take(out, pos[n_tok:])
                guest = seen.astype(jnp.bfloat16)
                back = hop(guest, lend[l])
                home_again = lambda: take(back, place)
                if l + 1 < n_layers:
                    late = after(full[NG - 1], guest)
                else:
                    returned = home_again()
                    late = after(full[NG - 1], guest, returned)
                    home_again = lambda: returned
                out = gathered(NG - 1, out, late)
                mixed = (acc[:n_tok] + g1[:n_tok] * take(out, pos[:n_tok])).astype(jnp.bfloat16)
                x = jnp.where(my_lent[l][:, None], home_again(), mixed)
                if l + 1 < n_layers:
                    x, own_x, sent = lax.optimization_barrier((x, own_x2, sent2))
                    full, own = coming, own2
            return x

        return lax.cond(ok, adaptive, general, tokens, norm_w, router_w, w_gate, w_up, w_down, ids)

    row_spec = P(("rep", "fsdp"), None)
    col_spec = P(None, None, None, "fsdp")
    return jax.shard_map(
        local_fn,
        mesh=mesh,
        in_specs=(row_spec, P(), P(), col_spec, col_spec, P(None, None, "fsdp", None), P(None, ("rep", "fsdp"), None)),
        out_specs=row_spec,
        check_vma=False,
    )
```

```python
import functools

import jax
import jax.numpy as jnp
from jax import lax
from jax.experimental import pallas as pl
from jax.experimental.pallas import tpu as pltpu
from jax.sharding import PartitionSpec as P


EPS = 1e-5
TM = 256
DC = 256
NG = 4
CAP = 256
SIDE_RANKS = {4: ((4, 7), (5, 6)), 2: ((2, 5, 7), (3, 4, 6))}
VMEM = 66 * 1000 * 1000


def pad16(n):
    return (n + 15) // 16 * 16


def prep_body(groups, n_exp, s_ref, *refs):
    srcs, outs, sel = refs[:3], refs[3:-1], refs[-1]
    n = sum(groups)
    wide = sel.shape[0] // n

    @pl.when(pl.program_id(0) == 0)
    def _():
        col = lax.broadcasted_iota(jnp.int32, (wide, sel.shape[1]), 1)
        line = lax.broadcasted_iota(jnp.int32, (wide, sel.shape[1]), 0)
        for k in range(n):
            sel[k * wide:(k + 1) * wide, :] = (col == line * n_exp + s_ref[k]).astype(jnp.bfloat16)

    for m in range(3):
        k = 0
        for out, size in zip(outs, groups):
            for j in range(size):
                out[j, m] = jnp.dot(sel[k * wide:(k + 1) * wide, :], srcs[m][0], preferred_element_type=jnp.float32).astype(jnp.bfloat16)
                k += 1


def prep(layer, experts, groups, w_gate, w_up, w_down):
    n_exp, width, inner = w_gate.shape[1:]
    wide = pad16(inner)
    lines = [jnp.transpose(w, order).reshape(w.shape[0], inner * n_exp, width) for w, order in ((w_gate, (0, 3, 1, 2)), (w_up, (0, 3, 1, 2)), (w_down, (0, 2, 1, 3)))]
    n = sum(groups)
    return pl.pallas_call(
        functools.partial(prep_body, groups, n_exp),
        out_shape=[jax.ShapeDtypeStruct((g, 3, wide, width), jnp.bfloat16) for g in groups],
        grid_spec=pltpu.PrefetchScalarGridSpec(
            num_scalar_prefetch=1,
            grid=(width // DC,),
            in_specs=[pl.BlockSpec((1, inner * n_exp, DC), lambda c, s: (layer, 0, c))] * 3,
            out_specs=[pl.BlockSpec((g, 3, wide, DC), lambda c, s: (0, 0, 0, c)) for g in groups],
            scratch_shapes=[pltpu.VMEM((n * wide, inner * n_exp), jnp.bfloat16)],
        ),
        compiler_params=pltpu.CompilerParams(vmem_limit_bytes=VMEM),
        cost_estimate=pl.CostEstimate(flops=n * 600_000_000, bytes_accessed=70_000_000 + n * 4_300_000, transcendentals=0),
        name="prep",
    )(experts, *lines)


def expert_body(pieces, n_w, aliased, added, s_ref, h_ref, *refs):
    w_refs = refs[:n_w]
    more = n_w + aliased + 2 * added
    o_ref = refs[more]
    w1, w3, w2, act, sems = refs[more + 1:]
    wide = w1.shape[0] // len(pieces)
    i = pl.program_id(0)

    def copies(m, dst):
        out = []
        for p, (r, lead) in enumerate(pieces):
            src = w_refs[r].at[lead + (m,)] if isinstance(lead, tuple) else w_refs[r].at[lead, m]
            out.append(pltpu.make_async_copy(src, dst.at[pl.ds(p * wide, wide)], sems.at[m, p]))
        return out

    @pl.when(i == 0)
    def _():
        for m, dst in enumerate((w1, w3, w2)):
            for c in copies(m, dst):
                c.start()
        for m, dst in enumerate((w1, w3)):
            for c in copies(m, dst):
                c.wait()

    nt = (((1,), (1,)), ((), ()))

    @pl.when(i < s_ref[1])
    def _():
        cols = w1.shape[0]
        steps = (cols + 255) // 256

        def up(c, carry):
            at = pl.multiple_of(jnp.minimum(c * 256, cols - 256), 128)
            h = h_ref[...]
            u = lax.dot_general(h, w1[pl.ds(at, 256), :], nt, preferred_element_type=jnp.float32)
            v = lax.dot_general(h, w3[pl.ds(at, 256), :], nt, preferred_element_type=jnp.float32)
            act[:, pl.ds(at, 256)] = (jax.nn.silu(u) * v).astype(jnp.bfloat16)
            return carry

        lax.fori_loop(0, steps, up, 0)

    @pl.when(i == 0)
    def _():
        for c in copies(2, w2):
            c.wait()

    @pl.when(i < s_ref[1])
    def _():
        def down(c, carry):
            at = pl.multiple_of(c * 512, 512)
            o = jnp.dot(act[...], w2[:, pl.ds(at, 512)], preferred_element_type=jnp.float32)
            if added:
                x_ref, gate_ref = refs[more - 2:more]
                o = x_ref[:, pl.ds(at, 512)].astype(jnp.float32) + gate_ref[...] * o
            o_ref[:, pl.ds(at, 512)] = o
            return carry

        lax.fori_loop(0, o_ref.shape[1] // 512, down, 0)


def expert(scalars, rows, weights, pieces, out, max_tiles, add=None):
    width = rows.shape[1]
    wide = weights[0].shape[-2]
    cols = wide * len(pieces)
    aliased = out is not None
    at = lambda i, s: (s[0] + jnp.minimum(i, s[1] - 1), 0)
    anywhere = pl.BlockSpec(memory_space=pl.ANY)
    return pl.pallas_call(
        functools.partial(expert_body, pieces, len(weights), aliased, add is not None),
        out_shape=jax.ShapeDtypeStruct(rows.shape, jnp.float32),
        grid_spec=pltpu.PrefetchScalarGridSpec(
            num_scalar_prefetch=1,
            grid=(max_tiles,),
            in_specs=[pl.BlockSpec((TM, width), at)] + [anywhere] * (len(weights) + aliased)
            + ([pl.BlockSpec((TM, width), at), pl.BlockSpec((TM, 1), at)] if add else []),
            out_specs=pl.BlockSpec((TM, width), at),
            scratch_shapes=[pltpu.VMEM((cols, width), jnp.bfloat16)] * 3
            + [pltpu.VMEM((TM, cols), jnp.bfloat16), pltpu.SemaphoreType.DMA((3, len(pieces)))],
        ),
        input_output_aliases={2 + len(weights): 0} if aliased else {},
        compiler_params=pltpu.CompilerParams(vmem_limit_bytes=VMEM),
        cost_estimate=pl.CostEstimate(flops=3_000_000_000, bytes_accessed=60_000_000, transcendentals=0),
        name="expert",
    )(scalars, rows, *weights, *((out,) if aliased else ()), *(add or ()))


def prefix(onehot):
    n, k = onehot.shape
    blocks = onehot.astype(jnp.float32).reshape(n // 128, 128, k)
    lower = (jnp.arange(128)[:, None] > jnp.arange(128)[None, :]).astype(jnp.float32)
    inside = jnp.einsum("ij,bjk->bik", lower, blocks)
    sums = blocks.sum(axis=1)
    nb = n // 128
    before = jnp.einsum("ij,jk->ik", (jnp.arange(nb)[:, None] > jnp.arange(nb)[None, :]).astype(jnp.float32), sums)
    return (inside + before[:, None, :]).reshape(n, k).astype(jnp.int32), sums.sum(axis=0).astype(jnp.int32)


def row_plan(slots, n_local):
    n = slots.shape[0]
    onehot = slots[:, None] == jnp.arange(n_local)[None, :]
    within, counts = prefix(onehot)
    tiles = jnp.maximum((counts + TM - 1) // TM, 1)
    lower = jnp.arange(n_local)[:, None] > jnp.arange(n_local)[None, :]
    first = jnp.sum(jnp.where(lower, tiles[None, :], 0), axis=1)
    pos = jnp.sum(jnp.where(onehot, within + first[None, :] * TM, 0), axis=1)
    spare = jnp.where(jnp.arange(TM)[None, :] < (tiles * TM - counts)[:, None], jnp.arange(n_local)[:, None], n_local)
    keys = jnp.concatenate([slots, spare.reshape(-1)])
    order = lax.sort(keys * 8192 + jnp.arange(keys.shape[0], dtype=jnp.int32)) & 8191
    scalars = jnp.stack([first, tiles], axis=1).astype(jnp.int32)
    return jnp.where(order < n, order, 0), pos, scalars


def pick(table, index, size):
    return jnp.sum(jnp.where(index[..., None] == jnp.arange(size), table, 0), axis=-1)


def norm_gates(x, norm_w, router_w, ids0, ids1):
    xf = x.astype(jnp.float32)
    inv = lax.rsqrt(jnp.mean(xf * xf, axis=-1, keepdims=True) + EPS)
    h = (xf * inv * norm_w).astype(jnp.bfloat16)
    r = jnp.dot(h, router_w, preferred_element_type=jnp.float32)
    n_exp = router_w.shape[1]
    r0 = jnp.sum(jnp.where(ids0[:, None] == jnp.arange(n_exp), r, 0.0), axis=-1)
    r1 = jnp.sum(jnp.where(ids1[:, None] == jnp.arange(n_exp), r, 0.0), axis=-1)
    g = jax.nn.softmax(jnp.stack([r0, r1], axis=-1), axis=-1)
    return h, g[:, :1], g[:, 1:]


def take(table, index):
    return table.at[index].get(mode="promise_in_bounds")


def solution(mesh):
    n_dev = mesh.shape["fsdp"]

    def hop(a, bit):
        return lax.ppermute(a, "fsdp", [(i, i ^ bit) for i in range(n_dev)])

    def general(x, norm_w, router_w, w_gate, w_up, w_down, ids):
        n_layers, n_exp = w_gate.shape[:2]
        n_tok = x.shape[0]
        for l in range(n_layers):
            slot, pos, scalars = row_plan(jnp.concatenate([ids[l, 0], ids[l, 1]]), n_exp)
            h, g0, g1 = norm_gates(x, norm_w[l], router_w[l], ids[l, 0], ids[l, 1])
            rows = take(h, slot % n_tok)

            def step(e, out, l=l, rows=rows, scalars=scalars):
                w = prep(l, e[None].astype(jnp.int32), (1,), w_gate, w_up, w_down)[0][0]
                full = lax.all_gather(w, "fsdp")
                s = lax.dynamic_index_in_dim(scalars, e, 0, keepdims=False)
                return expert(s, rows, [full], [(0, p) for p in range(n_dev)], out, n_tok // TM)

            out = lax.fori_loop(0, n_exp, step, jnp.zeros(rows.shape, jnp.float32))
            x = (x.astype(jnp.float32) + (g0 * take(out, pos[:n_tok]) + g1 * take(out, pos[n_tok:]))).astype(jnp.bfloat16)
        return x

    def local_fn(tokens, norm_w, router_w, w_gate, w_up, w_down, route_ids):
        n_layers, n_exp = w_gate.shape[:2]
        n_tok = tokens.shape[0]
        n_light = (n_exp - NG) // 2
        n_local = NG + n_light
        me = lax.axis_index("fsdp")
        ids = jnp.swapaxes(route_ids, 1, 2)
        every = lax.all_gather(ids, "fsdp")
        hits = every[..., None] == jnp.arange(n_exp)
        load = jnp.sum(hits.astype(jnp.int32), axis=(0, 2, 3))
        earlier = jnp.arange(n_exp)[None, :] < jnp.arange(n_exp)[:, None]
        ahead = (load[:, None, :] > load[:, :, None]) | ((load[:, None, :] == load[:, :, None]) & earlier[None])
        rank = jnp.sum(ahead.astype(jnp.int32), axis=2)
        by_rank = jnp.sum(jnp.where(rank[:, None, :] == jnp.arange(n_exp)[None, :, None], jnp.arange(n_exp), 0), axis=2).astype(jnp.int32)
        home_of = [-1] * NG + [0] * (n_exp - NG)
        local_of = list(range(n_exp))
        for side, ranks in enumerate(SIDE_RANKS[NG]):
            for j, k in enumerate(ranks):
                home_of[k], local_of[k] = side, NG + j
        home = pick(jnp.array(home_of), rank, n_exp)
        local = pick(jnp.array(local_of), rank, n_exp)
        at_home = jnp.sum(jnp.where(hits, home[None, :, None, None, :], 0), axis=-1)
        lend = [n_dev // 2 if l % 2 == 0 else n_dev // 4 for l in range(n_layers)]
        share = [n_dev // 4 if l % 2 == 0 else n_dev // 2 for l in range(n_layers)]
        side_of = jnp.stack([(jnp.arange(n_dev) // bit) % 2 for bit in lend], axis=1)
        mine_side = jnp.stack([(me // bit) % 2 for bit in lend])
        needs = [jnp.any(at_home == v, axis=2) for v in (0, 1)]
        top = jnp.sum(jnp.where(rank == 0, jnp.arange(n_exp), 0), axis=1)[None, :, None, None]
        shared = jnp.all(jnp.any(every == top, axis=2))
        lent = jnp.where(side_of[:, :, None] == 0, needs[1], needs[0])
        n_lent = jnp.sum(lent.astype(jnp.int32), axis=2)
        ok = jnp.all(n_lent <= CAP) & shared

        def adaptive(x, norm_w, router_w, w_gate, w_up, w_down, ids):
            mine = lax.dynamic_index_in_dim(every, me, 0, keepdims=False)
            my_lent = lax.dynamic_index_in_dim(lent, me, 0, keepdims=False)
            my_top = jnp.sum(jnp.where(rank == 0, jnp.arange(n_exp), 0), axis=1)
            mine = jnp.where(mine[:, 0] == my_top[:, None], mine[:, 1], mine[:, 0])
            my_local = pick(local[:, None, :], mine, n_exp)
            sides = [jnp.array(r) for r in SIDE_RANKS[NG]]
            chosen = [[jnp.where(mine_side[l] == v, by_rank[l][sides[0]], by_rank[l][sides[1]]) for v in (0, 1)] for l in range(n_layers)]

            picks = [(by_rank[l, :1], jnp.concatenate([by_rank[l, 1:NG], *chosen[l]])) for l in range(n_layers)]
            picks = lax.optimization_barrier(picks)

            def shards(l, top, others):
                first = prep(l, top, (1,), w_gate, w_up, w_down)
                rest = prep(l, others, (1,) * (NG - 1 + 2 * n_light), w_gate, w_up, w_down)
                rest = [w[0] for w in rest]
                return first[0][0], rest[:NG - 1], rest[NG - 1:NG - 1 + n_light], rest[NG - 1 + n_light:]

            def all_of(w):
                return lax.all_gather(w, "fsdp")

            def after(values, *waited):
                return lax.optimization_barrier((values, *waited))[0]

            top_w, heavy_w, own, other = shards(0, *picks[0])
            full = [all_of(top_w)] + [all_of(w) for w in heavy_w]
            lists = []
            for l in range(n_layers):
                key = jnp.where(my_lent[l], 0, 8192) + jnp.arange(n_tok, dtype=jnp.int32)
                key, code = lax.sort((key, jnp.where(my_lent[l], my_local[l] * 8 + mine[l], n_local * 8)), num_keys=1)
                place = jnp.minimum(prefix(my_lent[l][:, None])[0][:, 0], CAP - 1)
                code = hop(code[:CAP], lend[l])
                lists.append(((key & 8191)[:CAP], place, code))
            for l in range(n_layers):
                key, place, code = lists[l]
                guest = hop(take(x, key), lend[l])
                if l == 0:
                    own_x, sent = [hop(w, share[0]) for w in own], [hop(w, lend[0]) for w in other]
                both = jnp.concatenate([x, guest])
                ids1 = jnp.concatenate([mine[l], code % 8])
                slots = jnp.concatenate([jnp.where(my_lent[l], n_local, my_local[l]), code // 8]) - 1
                slots = jnp.where(slots < 0, n_local - 1, slots)
                token, pos, scalars = row_plan(slots, n_local - 1)
                h, g0, g1 = norm_gates(both, norm_w[l], router_w[l], jnp.broadcast_to(my_top[l], ids1.shape), ids1)
                rows = take(h, token)
                max_tiles = (n_tok + CAP) // TM
                whole = [(0, p) for p in range(n_dev)]
                gathered = lambda k, out, w: expert(scalars[k - 1], rows, [w], whole, out, max_tiles)
                if l:
                    far = [hop(w, share[l]) for w in sent]
                    beside = [[hop(w, 1) for w in ws] for ws in zip(own, own_x, sent)]
                acc = expert(jnp.array([0, max_tiles], jnp.int32), h, [full[0]], whole, None, max_tiles, add=(both, g0))
                rows = after(rows, acc)
                if l == 0:
                    own_x, sent = after((own_x, sent), acc)
                    far = [hop(w, share[l]) for w in sent]
                    beside = [[hop(w, 1) for w in ws] for ws in zip(own, own_x, sent)]
                if l + 1 < n_layers:
                    top_w, heavy_w, own2, other2 = shards(l + 1, *after(picks[l + 1], acc))
                    coming = [all_of(top_w)] + [all_of(w) for w in heavy_w]
                    own_x2, sent2 = [hop(w, share[l + 1]) for w in own2], [hop(w, lend[l + 1]) for w in other2]
                out = None
                early = NG - 1 if l + 1 < n_layers else min(2, NG - 1)
                for k in range(1, early):
                    out = gathered(k, out, full[k])
                far = after(far, acc if out is None else out)
                for j in range(n_light):
                    w8 = [own[j], own_x[j], sent[j], far[j]] + beside[j] + [hop(far[j], 1)]
                    out = expert(scalars[NG - 1 + j], rows, w8, [(p, ()) for p in range(n_dev)], out, max_tiles)
                seen = acc[n_tok:] + g1[n_tok:] * take(out, pos[n_tok:])
                guest = seen.astype(jnp.bfloat16)
                back = hop(guest, lend[l])
                for k in range(early, NG - 1):
                    out = gathered(k, out, after(full[k], guest))
                home_again = lambda: take(back, place)
                if l + 1 < n_layers:
                    late = after(full[NG - 1], guest)
                else:
                    returned = home_again()
                    late = after(full[NG - 1], out, returned)
                    home_again = lambda: returned
                out = gathered(NG - 1, out, late)
                mixed = (acc[:n_tok] + g1[:n_tok] * take(out, pos[:n_tok])).astype(jnp.bfloat16)
                x = jnp.where(my_lent[l][:, None], home_again(), mixed)
                if l + 1 < n_layers:
                    x, own_x, sent = lax.optimization_barrier((x, own_x2, sent2))
                    full, own = coming, own2
            return x

        return lax.cond(ok, adaptive, general, tokens, norm_w, router_w, w_gate, w_up, w_down, ids)

    row_spec = P(("rep", "fsdp"), None)
    col_spec = P(None, None, None, "fsdp")
    return jax.shard_map(
        local_fn,
        mesh=mesh,
        in_specs=(row_spec, P(), P(), col_spec, col_spec, P(None, None, "fsdp", None), P(None, ("rep", "fsdp"), None)),
        out_specs=row_spec,
        check_vma=False,
    )
```

```python
import functools

import jax
import jax.numpy as jnp
from jax import lax
from jax.experimental import pallas as pl
from jax.experimental.pallas import tpu as pltpu
from jax.sharding import PartitionSpec as P


EPS = 1e-5
TM = 256
DC = 256
NG = 4
CAP = 320
SIDE_RANKS = {4: ((4, 7), (5, 6)), 2: ((2, 5, 7), (3, 4, 6))}
VMEM = 66 * 1000 * 1000


def pad16(n):
    return (n + 15) // 16 * 16


def prep_body(groups, n_exp, s_ref, *refs):
    srcs, outs, sel = refs[:3], refs[3:-1], refs[-1]
    n = sum(groups)
    wide = sel.shape[0] // n

    @pl.when(pl.program_id(0) == 0)
    def _():
        col = lax.broadcasted_iota(jnp.int32, (wide, sel.shape[1]), 1)
        line = lax.broadcasted_iota(jnp.int32, (wide, sel.shape[1]), 0)
        for k in range(n):
            sel[k * wide:(k + 1) * wide, :] = (col == line * n_exp + s_ref[k]).astype(jnp.bfloat16)

    for m in range(3):
        k = 0
        for out, size in zip(outs, groups):
            for j in range(size):
                out[j, m] = jnp.dot(sel[k * wide:(k + 1) * wide, :], srcs[m][0], preferred_element_type=jnp.float32).astype(jnp.bfloat16)
                k += 1


def prep(layer, experts, groups, w_gate, w_up, w_down):
    n_exp, width, inner = w_gate.shape[1:]
    wide = pad16(inner)
    lines = [jnp.transpose(w, order).reshape(w.shape[0], inner * n_exp, width) for w, order in ((w_gate, (0, 3, 1, 2)), (w_up, (0, 3, 1, 2)), (w_down, (0, 2, 1, 3)))]
    n = sum(groups)
    return pl.pallas_call(
        functools.partial(prep_body, groups, n_exp),
        out_shape=[jax.ShapeDtypeStruct((g, 3, wide, width), jnp.bfloat16) for g in groups],
        grid_spec=pltpu.PrefetchScalarGridSpec(
            num_scalar_prefetch=1,
            grid=(width // DC,),
            in_specs=[pl.BlockSpec((1, inner * n_exp, DC), lambda c, s: (layer, 0, c))] * 3,
            out_specs=[pl.BlockSpec((g, 3, wide, DC), lambda c, s: (0, 0, 0, c)) for g in groups],
            scratch_shapes=[pltpu.VMEM((n * wide, inner * n_exp), jnp.bfloat16)],
        ),
        compiler_params=pltpu.CompilerParams(vmem_limit_bytes=VMEM),
        cost_estimate=pl.CostEstimate(flops=n * 600_000_000, bytes_accessed=70_000_000 + n * 4_300_000, transcendentals=0),
        name="prep",
    )(experts, *lines)


def expert_body(pieces, n_w, aliased, added, s_ref, h_ref, *refs):
    w_refs = refs[:n_w]
    more = n_w + aliased + 2 * added
    o_ref = refs[more]
    w1, w3, w2, act, sems = refs[more + 1:]
    wide = w1.shape[0] // len(pieces)
    i = pl.program_id(0)

    def copies(m, dst):
        out = []
        for p, (r, lead) in enumerate(pieces):
            src = w_refs[r].at[lead + (m,)] if isinstance(lead, tuple) else w_refs[r].at[lead, m]
            out.append(pltpu.make_async_copy(src, dst.at[pl.ds(p * wide, wide)], sems.at[m, p]))
        return out

    @pl.when(i == 0)
    def _():
        for m, dst in enumerate((w1, w3, w2)):
            for c in copies(m, dst):
                c.start()
        for m, dst in enumerate((w1, w3)):
            for c in copies(m, dst):
                c.wait()

    nt = (((1,), (1,)), ((), ()))

    @pl.when(i < s_ref[1])
    def _():
        cols = w1.shape[0]
        steps = (cols + 255) // 256

        def up(c, carry):
            at = pl.multiple_of(jnp.minimum(c * 256, cols - 256), 128)
            h = h_ref[...]
            u = lax.dot_general(h, w1[pl.ds(at, 256), :], nt, preferred_element_type=jnp.float32)
            v = lax.dot_general(h, w3[pl.ds(at, 256), :], nt, preferred_element_type=jnp.float32)
            act[:, pl.ds(at, 256)] = (jax.nn.silu(u) * v).astype(jnp.bfloat16)
            return carry

        lax.fori_loop(0, steps, up, 0)

    @pl.when(i == 0)
    def _():
        for c in copies(2, w2):
            c.wait()

    @pl.when(i < s_ref[1])
    def _():
        def down(c, carry):
            at = pl.multiple_of(c * 512, 512)
            o = jnp.dot(act[...], w2[:, pl.ds(at, 512)], preferred_element_type=jnp.float32)
            if added:
                x_ref, gate_ref = refs[more - 2:more]
                o = x_ref[:, pl.ds(at, 512)].astype(jnp.float32) + gate_ref[...] * o
            o_ref[:, pl.ds(at, 512)] = o
            return carry

        lax.fori_loop(0, o_ref.shape[1] // 512, down, 0)


def expert(scalars, rows, weights, pieces, out, max_tiles, add=None):
    width = rows.shape[1]
    wide = weights[0].shape[-2]
    cols = wide * len(pieces)
    aliased = out is not None
    at = lambda i, s: (s[0] + jnp.minimum(i, s[1] - 1), 0)
    anywhere = pl.BlockSpec(memory_space=pl.ANY)
    return pl.pallas_call(
        functools.partial(expert_body, pieces, len(weights), aliased, add is not None),
        out_shape=jax.ShapeDtypeStruct(rows.shape, jnp.float32),
        grid_spec=pltpu.PrefetchScalarGridSpec(
            num_scalar_prefetch=1,
            grid=(max_tiles,),
            in_specs=[pl.BlockSpec((TM, width), at)] + [anywhere] * (len(weights) + aliased)
            + ([pl.BlockSpec((TM, width), at), pl.BlockSpec((TM, 1), at)] if add else []),
            out_specs=pl.BlockSpec((TM, width), at),
            scratch_shapes=[pltpu.VMEM((cols, width), jnp.bfloat16)] * 3
            + [pltpu.VMEM((TM, cols), jnp.bfloat16), pltpu.SemaphoreType.DMA((3, len(pieces)))],
        ),
        input_output_aliases={2 + len(weights): 0} if aliased else {},
        compiler_params=pltpu.CompilerParams(vmem_limit_bytes=VMEM),
        cost_estimate=pl.CostEstimate(flops=3_000_000_000, bytes_accessed=60_000_000, transcendentals=0),
        name="expert",
    )(scalars, rows, *weights, *((out,) if aliased else ()), *(add or ()))


def prefix(onehot):
    n, k = onehot.shape
    blocks = onehot.astype(jnp.float32).reshape(n // 128, 128, k)
    lower = (jnp.arange(128)[:, None] > jnp.arange(128)[None, :]).astype(jnp.float32)
    inside = jnp.einsum("ij,bjk->bik", lower, blocks)
    sums = blocks.sum(axis=1)
    nb = n // 128
    before = jnp.einsum("ij,jk->ik", (jnp.arange(nb)[:, None] > jnp.arange(nb)[None, :]).astype(jnp.float32), sums)
    return (inside + before[:, None, :]).reshape(n, k).astype(jnp.int32), sums.sum(axis=0).astype(jnp.int32)


def row_plan(slots, n_local):
    n = slots.shape[0]
    slots = jnp.concatenate([slots, jnp.full(-n % 128, n_local, slots.dtype)])
    onehot = slots[:, None] == jnp.arange(n_local)[None, :]
    within, counts = prefix(onehot)
    tiles = jnp.maximum((counts + TM - 1) // TM, 1)
    lower = jnp.arange(n_local)[:, None] > jnp.arange(n_local)[None, :]
    first = jnp.sum(jnp.where(lower, tiles[None, :], 0), axis=1)
    pos = jnp.sum(jnp.where(onehot, within + first[None, :] * TM, 0), axis=1)
    spare = jnp.where(jnp.arange(TM)[None, :] < (tiles * TM - counts)[:, None], jnp.arange(n_local)[:, None], n_local)
    keys = jnp.concatenate([slots, spare.reshape(-1)])
    order = lax.sort(keys * 8192 + jnp.arange(keys.shape[0], dtype=jnp.int32)) & 8191
    scalars = jnp.stack([first, tiles], axis=1).astype(jnp.int32)
    return jnp.where(order < n, order, 0), pos[:n], scalars


def pick(table, index, size):
    return jnp.sum(jnp.where(index[..., None] == jnp.arange(size), table, 0), axis=-1)


def norm_gates(x, norm_w, router_w, ids0, ids1):
    xf = x.astype(jnp.float32)
    inv = lax.rsqrt(jnp.mean(xf * xf, axis=-1, keepdims=True) + EPS)
    h = (xf * inv * norm_w).astype(jnp.bfloat16)
    r = jnp.dot(h, router_w, preferred_element_type=jnp.float32)
    n_exp = router_w.shape[1]
    r0 = jnp.sum(jnp.where(ids0[:, None] == jnp.arange(n_exp), r, 0.0), axis=-1)
    r1 = jnp.sum(jnp.where(ids1[:, None] == jnp.arange(n_exp), r, 0.0), axis=-1)
    g = jax.nn.softmax(jnp.stack([r0, r1], axis=-1), axis=-1)
    return h, g[:, :1], g[:, 1:]


def take(table, index):
    return table.at[index].get(mode="promise_in_bounds")


def solution(mesh):
    n_dev = mesh.shape["fsdp"]

    def hop(a, bit):
        return lax.ppermute(a, "fsdp", [(i, i ^ bit) for i in range(n_dev)])

    def general(x, norm_w, router_w, w_gate, w_up, w_down, ids):
        n_layers, n_exp = w_gate.shape[:2]
        n_tok = x.shape[0]
        for l in range(n_layers):
            slot, pos, scalars = row_plan(jnp.concatenate([ids[l, 0], ids[l, 1]]), n_exp)
            h, g0, g1 = norm_gates(x, norm_w[l], router_w[l], ids[l, 0], ids[l, 1])
            rows = take(h, slot % n_tok)

            def step(e, out, l=l, rows=rows, scalars=scalars):
                w = prep(l, e[None].astype(jnp.int32), (1,), w_gate, w_up, w_down)[0][0]
                full = lax.all_gather(w, "fsdp")
                s = lax.dynamic_index_in_dim(scalars, e, 0, keepdims=False)
                return expert(s, rows, [full], [(0, p) for p in range(n_dev)], out, n_tok // TM)

            out = lax.fori_loop(0, n_exp, step, jnp.zeros(rows.shape, jnp.float32))
            x = (x.astype(jnp.float32) + (g0 * take(out, pos[:n_tok]) + g1 * take(out, pos[n_tok:]))).astype(jnp.bfloat16)
        return x

    def local_fn(tokens, norm_w, router_w, w_gate, w_up, w_down, route_ids):
        n_layers, n_exp = w_gate.shape[:2]
        n_tok = tokens.shape[0]
        n_light = (n_exp - NG) // 2
        n_local = NG + n_light
        me = lax.axis_index("fsdp")
        ids = jnp.swapaxes(route_ids, 1, 2)
        every = lax.all_gather(ids, "fsdp")
        hits = every[..., None] == jnp.arange(n_exp)
        load = jnp.sum(hits.astype(jnp.int32), axis=(0, 2, 3))
        earlier = jnp.arange(n_exp)[None, :] < jnp.arange(n_exp)[:, None]
        ahead = (load[:, None, :] > load[:, :, None]) | ((load[:, None, :] == load[:, :, None]) & earlier[None])
        rank = jnp.sum(ahead.astype(jnp.int32), axis=2)
        by_rank = jnp.sum(jnp.where(rank[:, None, :] == jnp.arange(n_exp)[None, :, None], jnp.arange(n_exp), 0), axis=2).astype(jnp.int32)
        home_of = [-1] * NG + [0] * (n_exp - NG)
        local_of = list(range(n_exp))
        for side, ranks in enumerate(SIDE_RANKS[NG]):
            for j, k in enumerate(ranks):
                home_of[k], local_of[k] = side, NG + j
        home = pick(jnp.array(home_of), rank, n_exp)
        local = pick(jnp.array(local_of), rank, n_exp)
        at_home = jnp.sum(jnp.where(hits, home[None, :, None, None, :], 0), axis=-1)
        lend = [n_dev // 2 if l % 2 == 0 else n_dev // 4 for l in range(n_layers)]
        share = [n_dev // 4 if l % 2 == 0 else n_dev // 2 for l in range(n_layers)]
        side_of = jnp.stack([(jnp.arange(n_dev) // bit) % 2 for bit in lend], axis=1)
        mine_side = jnp.stack([(me // bit) % 2 for bit in lend])
        needs = [jnp.any(at_home == v, axis=2) for v in (0, 1)]
        top = jnp.sum(jnp.where(rank == 0, jnp.arange(n_exp), 0), axis=1)[None, :, None, None]
        shared = jnp.all(jnp.any(every == top, axis=2))
        lent = jnp.where(side_of[:, :, None] == 0, needs[1], needs[0])
        n_lent = jnp.sum(lent.astype(jnp.int32), axis=2)
        ok = jnp.all(n_lent <= CAP) & shared

        def adaptive(x, norm_w, router_w, w_gate, w_up, w_down, ids):
            mine = lax.dynamic_index_in_dim(every, me, 0, keepdims=False)
            my_lent = lax.dynamic_index_in_dim(lent, me, 0, keepdims=False)
            my_top = jnp.sum(jnp.where(rank == 0, jnp.arange(n_exp), 0), axis=1)
            mine = jnp.where(mine[:, 0] == my_top[:, None], mine[:, 1], mine[:, 0])
            my_local = pick(local[:, None, :], mine, n_exp)
            sides = [jnp.array(r) for r in SIDE_RANKS[NG]]
            chosen = [[jnp.where(mine_side[l] == v, by_rank[l][sides[0]], by_rank[l][sides[1]]) for v in (0, 1)] for l in range(n_layers)]

            picks = [(by_rank[l, :1], jnp.concatenate([by_rank[l, 1:NG], *chosen[l]])) for l in range(n_layers)]
            picks = lax.optimization_barrier(picks)

            def shards(l, top, others):
                first = prep(l, top, (1,), w_gate, w_up, w_down)
                rest = prep(l, others, (1,) * (NG - 1 + 2 * n_light), w_gate, w_up, w_down)
                rest = [w[0] for w in rest]
                return first[0][0], rest[:NG - 1], rest[NG - 1:NG - 1 + n_light], rest[NG - 1 + n_light:]

            def all_of(w):
                return lax.all_gather(w, "fsdp")

            def after(values, *waited):
                return lax.optimization_barrier((values, *waited))[0]

            top_w, heavy_w, own, other = shards(0, *picks[0])
            full = [all_of(top_w)] + [all_of(w) for w in heavy_w]
            lists = []
            for l in range(n_layers):
                key = jnp.where(my_lent[l], 0, 8192) + jnp.arange(n_tok, dtype=jnp.int32)
                key, code = lax.sort((key, jnp.where(my_lent[l], my_local[l] * 8 + mine[l], n_local * 8)), num_keys=1)
                place = jnp.minimum(prefix(my_lent[l][:, None])[0][:, 0], CAP - 1)
                code = hop(code[:CAP], lend[l])
                lists.append(((key & 8191)[:CAP], place, code))
            for l in range(n_layers):
                key, place, code = lists[l]
                guest = hop(take(x, key), lend[l])
                if l == 0:
                    own_x, sent = [hop(w, share[0]) for w in own], [hop(w, lend[0]) for w in other]
                both = jnp.concatenate([x, guest])
                ids1 = jnp.concatenate([mine[l], code % 8])
                slots = jnp.concatenate([jnp.where(my_lent[l], n_local, my_local[l]), code // 8]) - 1
                slots = jnp.where(slots < 0, n_local - 1, slots)
                token, pos, scalars = row_plan(slots, n_local - 1)
                h, g0, g1 = norm_gates(both, norm_w[l], router_w[l], jnp.broadcast_to(my_top[l], ids1.shape), ids1)
                rows = take(h, token)
                max_tiles = pl.cdiv(n_tok + CAP, TM)
                whole = [(0, p) for p in range(n_dev)]
                gathered = lambda k, out, w: expert(scalars[k - 1], rows, [w], whole, out, max_tiles)
                if l:
                    far = [hop(w, share[l]) for w in sent]
                    beside = [[hop(w, 1) for w in ws] for ws in zip(own, own_x, sent)]
                acc = expert(jnp.array([0, max_tiles], jnp.int32), h, [full[0]], whole, None, max_tiles, add=(both, g0))
                rows = after(rows, acc)
                if l == 0:
                    own_x, sent = after((own_x, sent), acc)
                    far = [hop(w, share[l]) for w in sent]
                    beside = [[hop(w, 1) for w in ws] for ws in zip(own, own_x, sent)]
                if l + 1 < n_layers:
                    top_w, heavy_w, own2, other2 = shards(l + 1, *after(picks[l + 1], acc))
                    coming = [all_of(top_w)] + [all_of(w) for w in heavy_w]
                    own_x2, sent2 = [hop(w, share[l + 1]) for w in own2], [hop(w, lend[l + 1]) for w in other2]
                out = None
                early = NG - 1 if l + 1 < n_layers else min(2, NG - 1)
                for k in range(1, early):
                    out = gathered(k, out, full[k])
                far = after(far, acc if out is None else out)
                for j in range(n_light):
                    w8 = [own[j], own_x[j], sent[j], far[j]] + beside[j] + [hop(far[j], 1)]
                    out = expert(scalars[NG - 1 + j], rows, w8, [(p, ()) for p in range(n_dev)], out, max_tiles)
                seen = acc[n_tok:] + g1[n_tok:] * take(out, pos[n_tok:])
                guest = seen.astype(jnp.bfloat16)
                back = hop(guest, lend[l])
                for k in range(early, NG - 1):
                    out = gathered(k, out, after(full[k], guest))
                home_again = lambda: take(back, place)
                if l + 1 < n_layers:
                    late = after(full[NG - 1], guest)
                else:
                    returned = home_again()
                    late = after(full[NG - 1], out, returned)
                    home_again = lambda: returned
                out = gathered(NG - 1, out, late)
                mixed = (acc[:n_tok] + g1[:n_tok] * take(out, pos[:n_tok])).astype(jnp.bfloat16)
                x = jnp.where(my_lent[l][:, None], home_again(), mixed)
                if l + 1 < n_layers:
                    x, own_x, sent = lax.optimization_barrier((x, own_x2, sent2))
                    full, own = coming, own2
            return x

        return lax.cond(ok, adaptive, general, tokens, norm_w, router_w, w_gate, w_up, w_down, ids)

    row_spec = P(("rep", "fsdp"), None)
    col_spec = P(None, None, None, "fsdp")
    return jax.shard_map(
        local_fn,
        mesh=mesh,
        in_specs=(row_spec, P(), P(), col_spec, col_spec, P(None, None, "fsdp", None), P(None, ("rep", "fsdp"), None)),
        out_specs=row_spec,
        check_vma=False,
    )
```
